256 devices in a mesh: gx: 32 (over y, z), gy: 8 (over x, core).
Axes of the slice: x: 4, y: 4, z: 8, core: 2. Of those that a mesh axis runs over, the one named last changes fastest.
Arguments:
- modes: float32 [16, 3, 128, 64, 128], P(None, None, 'gx', 'gy'), may hold values from -0.03 to 0.03
- region: int32 [128, 64, 128], P('gx', 'gy'), may hold values from 0 to 15
- stiffness: float32 [16], replicated, may hold values from 0.1 to 10
- coarse_group: int32 [32, 8], replicated, may hold values from 0 to 3
Outputs:
- coarse: float32 [32, 64, 192], P('gx', 'gy')
The draws below stay inside these ranges and needn't reach their ends.
All inputs are finite; a program needn't handle non-finite values.
Results may differ from the reference program's by a relative error of at most 0.0003.
Values sent between devices are 32-bit elements; how exact they have to be, the bound alone decides.
No kernel may reach another device: no remote copies, remote signals or barrier semaphores. Data moves between devices by JAX's collectives and lax.ppermute only.
A program may use at most 128 MiB of HBM per device.

```python
import math
import jax
import jax.numpy as jnp
from jax import lax

MODES = 16
GROUPS = 4
REGIONS = 16
CX = 4
CY = 8
NZ = 128
NX = 128
NY = 64
N_GX = 32
N_GY = 8


def draw_modes(key, part):
    sigma = 0.0015
    wave_count = 4
    key_rough = jax.random.fold_in(key, 11)
    key_wave = jax.random.fold_in(key, 12)
    two_pi = 2.0 * math.pi
    freq_x = jax.random.uniform(jax.random.fold_in(key_wave, 1), (MODES, 3, wave_count), jnp.float32, 0.15, 0.6) * (two_pi / CX)
    freq_y = jax.random.uniform(jax.random.fold_in(key_wave, 2), (MODES, 3, wave_count), jnp.float32, 0.15, 0.6) * (two_pi / CY)
    freq_z = jax.random.uniform(jax.random.fold_in(key_wave, 3), (MODES, 3, wave_count), jnp.float32, 0.15, 0.6) * (two_pi / 16.0)
    sign_x = jax.random.rademacher(jax.random.fold_in(key_wave, 4), (MODES, 3, wave_count), jnp.float32)
    sign_y = jax.random.rademacher(jax.random.fold_in(key_wave, 5), (MODES, 3, wave_count), jnp.float32)
    phases = jax.random.uniform(jax.random.fold_in(key_wave, 6), (MODES, 3, wave_count), jnp.float32, 0.0, two_pi)
    freq_x = freq_x * sign_x
    freq_y = freq_y * sign_y
    amplitude = sigma / math.sqrt(0.5 * wave_count)
    coord_x = jnp.arange(NX, dtype=jnp.float32)[:, None, None]
    coord_y = jnp.arange(NY, dtype=jnp.float32)[None, :, None]
    coord_z = jnp.arange(NZ, dtype=jnp.float32)[None, None, :]

    def one_mode(index):
        key_mode = jax.random.fold_in(key_rough, index)
        noise = jax.random.truncated_normal(key_mode, -4.0, 4.0, (3, NX, NY, NZ), jnp.float32)
        for axis_num in (1, 2, 3):
            noise = noise + 0.6 * (jnp.roll(noise, 1, axis_num) + jnp.roll(noise, -1, axis_num))
        rough = noise * (sigma / 1.72 ** 1.5)
        mode_fx = freq_x[index]
        mode_fy = freq_y[index]
        mode_fz = freq_z[index]
        mode_phase = phases[index]
        comps = []
        for comp in range(3):
            total = jnp.zeros((NX, NY, NZ), jnp.float32)
            for wave in range(wave_count):
                angle_now = mode_fx[comp, wave] * coord_x + mode_fy[comp, wave] * coord_y + mode_fz[comp, wave] * coord_z + mode_phase[comp, wave]
                total = total + amplitude * jnp.cos(angle_now)
            comps.append(total)
        return rough + jnp.stack(comps)
    fields = lax.map(one_mode, jnp.arange(MODES, dtype=jnp.int32))
    return jnp.clip(fields, -0.029, 0.029)


def plant(entries, own_key, smallest, high):
    dims = entries.shape
    index_at = [jax.random.randint(jax.random.fold_in(own_key, axis), (), 0, dims[axis]) for axis in range(len(dims))]
    entries = entries.at[tuple(index_at)].set(smallest)
    longest = dims.index(max(dims))
    index_at[longest] = (index_at[longest] + 1) % dims[longest]
    return entries.at[tuple(index_at)].set(high)


def setup_inputs(seed: int = 0) -> dict:
    streams_of = jax.random.split(jax.random.key(seed), 5)
    modes = draw_modes(jax.random.fold_in(streams_of[4], 71), 0)
    region = plant(jax.random.randint(streams_of[1], (NX, NY, NZ), 0, REGIONS), jax.random.fold_in(streams_of[1], 1), 0, REGIONS - 1).astype(jnp.int32)
    stiffness = jnp.clip(jnp.exp(jax.random.uniform(streams_of[2], (REGIONS,), jnp.float32, math.log(0.1), math.log(10.0))), 0.1, 10.0)
    coarse_group = plant(jax.random.randint(streams_of[3], (N_GX, N_GY), 0, GROUPS), jax.random.fold_in(streams_of[3], 1), 0, GROUPS - 1).astype(jnp.int32)
    return dict(modes=modes, region=region, stiffness=stiffness, coarse_group=coarse_group)


beta_shear = 0.5
mass_share = 0.1


def all_offsets():
    return [(shift_x, shift_y, shift_z) for shift_x in (-1, 0, 1) for shift_y in (-1, 0, 1) for shift_z in (-1, 0, 1) if (shift_x, shift_y, shift_z) != (0, 0, 0)]


def apply_operator(padded, stiff_pad):
    span_x = padded.shape[2] - 2
    span_y = padded.shape[3] - 2
    span_z = padded.shape[4] - 2
    centre = padded[:, :, 1:span_x + 1, 1:span_y + 1, 1:span_z + 1]
    stiff_here = stiff_pad[1:span_x + 1, 1:span_y + 1, 1:span_z + 1]
    result = mass_share * stiff_here * centre
    for step_x, step_y, step_z in all_offsets():
        reach_len = abs(step_x) + abs(step_y) + abs(step_z)
        weight = 0.5 ** (reach_len - 1)
        nearby = padded[:, :, 1 + step_x:1 + step_x + span_x, 1 + step_y:1 + step_y + span_y, 1 + step_z:1 + step_z + span_z]
        stiff_there = stiff_pad[1 + step_x:1 + step_x + span_x, 1 + step_y:1 + step_y + span_y, 1 + step_z:1 + step_z + span_z]
        coupling = (0.5 * weight) * (stiff_here + stiff_there)
        differ = centre - nearby
        along_dir = (beta_shear / reach_len) * (step_x * differ[:, 0] + step_y * differ[:, 1] + step_z * differ[:, 2])
        pushed = differ + jnp.stack([step_x * along_dir, step_y * along_dir, step_z * along_dir], axis=1)
        result = result + coupling * pushed
    return result


def pair_blocks(applied, mode_cycle):
    span_x = mode_cycle.shape[2] - 2
    span_y = mode_cycle.shape[3] - 2
    bounds_x = [(0, 1), (1, span_x + 1), (span_x + 1, span_x + 2)]
    bounds_y = [(0, 1), (1, span_y + 1), (span_y + 1, span_y + 2)]
    rows_out = []
    for low_x, high_x in bounds_x:
        cols_out = []
        for low_y, high_y in bounds_y:
            cols_out.append(jnp.einsum('kaxyz,jaxyz->kj', applied[:, :, low_x:high_x, low_y:high_y], mode_cycle[:, :, low_x:high_x, low_y:high_y], precision=lax.Precision.HIGHEST))
        rows_out.append(jnp.stack(cols_out))
    return jnp.stack(rows_out)


def reference(modes, region, stiffness, coarse_group):
    stiff_cells = stiffness[region]
    cycle_pad = jnp.pad(modes, ((0, 0), (0, 0), (1, 1), (1, 1), (0, 0)))
    stiff_all = jnp.pad(stiff_cells, ((2, 2), (2, 2), (1, 1)))

    def one_block(sub_index):
        strip_row = (sub_index // N_GY).astype(jnp.int32)
        strip_col = (sub_index % N_GY).astype(jnp.int32)
        start_x = (strip_row * CX).astype(jnp.int32)
        start_y = (strip_col * CY).astype(jnp.int32)
        anchor = jnp.zeros((), jnp.int32)
        mode_cycle = lax.dynamic_slice(cycle_pad, (anchor, anchor, start_x, start_y, anchor), (MODES, 3, CX + 2, CY + 2, NZ))
        own_modes = lax.dynamic_slice(modes, (anchor, anchor, start_x, start_y, anchor), (MODES, 3, CX, CY, NZ))
        padded = jnp.pad(own_modes, ((0, 0), (0, 0), (2, 2), (2, 2), (1, 1)))
        stiff_pad = lax.dynamic_slice(stiff_all, (start_x, start_y, anchor), (CX + 4, CY + 4, NZ + 2))
        applied = apply_operator(padded, stiff_pad)
        return pair_blocks(applied, mode_cycle)

    blocks = lax.map(one_block, jnp.arange(N_GX * N_GY, dtype=jnp.int32))
    blocks = blocks.reshape(N_GX, N_GY, 3, 3, MODES, MODES)
    group_pad = jnp.pad(coarse_group, 1, constant_values=-1)
    near_groups = jnp.stack([jnp.stack([group_pad[1 + shift_x:1 + shift_x + N_GX, 1 + shift_y:1 + shift_y + N_GY] for shift_y in (-1, 0, 1)]) for shift_x in (-1, 0, 1)])
    labels = jnp.arange(GROUPS, dtype=jnp.int32)
    hot_near = (near_groups[..., None] == labels).astype(jnp.float32)
    hot_self = (coarse_group[..., None] == labels).astype(jnp.float32)
    coarse = jnp.einsum('abg,abxykj,xyabh->agkxhj', hot_self, blocks, hot_near, precision=lax.Precision.HIGHEST)
    return coarse.reshape(N_GX, GROUPS * MODES, 3 * GROUPS * MODES)
```

```python
import functools
import jax
import jax.numpy as jnp
from jax import lax
from jax.experimental import pallas as pl
from jax.experimental.pallas import tpu as pltpu
from jax.sharding import PartitionSpec as P

GROUPS = 4
MODES = 16
CX = 4
CY = 8
NZ = 128

beta_shear = 0.5
mass_share = 0.1

Q1 = 0.5 * beta_shear
Q2 = 0.25 * beta_shear / 2
Q3 = 0.125 * beta_shear / 3
DIAG = 7.0 + 2 * Q1 + 8 * Q2 + 8 * Q3
HALF = 0.5 * (mass_share + DIAG)

KZ = {(0, 0): (0.0, 0.5), (0, 1): (0.5, 0.25), (1, 0): (0.5, 0.25), (1, 1): (0.25, 0.125)}


def diag_weights(comp, ax, ay):
    c, s = KZ[(ax, ay)]
    m = ax + ay
    if (comp == 0 and ax) or (comp == 1 and ay):
        c += (0.0, Q1, Q2)[m]
        s += (Q1, Q2, Q3)[m]
    if comp == 2:
        s += (Q1, Q2, Q3)[m]
    return c, s


def add(*terms):
    terms = [t for t in terms if t is not None]
    if not terms:
        return None
    total = terms[0]
    for t in terms[1:]:
        total = total + t
    return total


def sub(a, b):
    if b is None:
        return a
    if a is None:
        return -b
    return a - b


def mul(k, a):
    return None if a is None or k == 0.0 else k * a


def z_parts(v):
    lane = lax.broadcasted_iota(jnp.int32, v.shape, 1)
    up = jnp.where(lane < NZ - 1, pltpu.roll(v, NZ - 1, 1), 0.0)
    down = jnp.where(lane > 0, pltpu.roll(v, 1, 1), 0.0)
    return v, up + down, up - down


NONE3 = (None, None, None)


def line(minus, centre, plus, want0=True, want1=True):
    minus, centre, plus = [(NONE3,) * 3 if t is None else t for t in (minus, centre, plus)]
    sum_c = [add(plus[i][0], minus[i][0]) for i in range(3)]
    sum_s = [add(plus[i][1], minus[i][1]) for i in range(3)]
    diff_dz = sub(plus[2][2], minus[2][2])
    diff_dy = sub(plus[1][2], minus[1][2])
    same, even, odd = [None] * 3, [None] * 3, [None] * 3
    for i in range(3):
        parts = (centre[i][0], centre[i][1], sum_c[i], sum_s[i])
        if want0:
            k = diag_weights(i, 0, 0) + diag_weights(i, 0, 1)
            same[i] = add(*[mul(w, t) for w, t in zip(k, parts)])
        if want1:
            k = diag_weights(i, 1, 0) + diag_weights(i, 1, 1)
            even[i] = add(*[mul(w, t) for w, t in zip(k, parts)])
    if want0:
        same[1] = add(same[1], mul(Q2, diff_dz))
        same[2] = add(same[2], mul(Q2, diff_dy))
    if want1:
        even[1] = add(even[1], mul(Q3, diff_dz))
        even[2] = add(even[2], mul(Q3, diff_dy))
        diff = [add(mul(Q2, sub(plus[i][0], minus[i][0])), mul(Q3, sub(plus[i][1], minus[i][1]))) for i in (0, 1)]
        odd[1] = diff[0]
        odd[0] = add(diff[1], mul(Q2, centre[2][2]), mul(Q3, add(plus[2][2], minus[2][2])))
        odd[2] = add(mul(Q2, centre[0][2]), mul(Q3, add(plus[0][2], minus[0][2])))
    return same, even, odd


def scalar_line(minus, centre, plus):
    minus, centre, plus = [NONE3 if t is None else t for t in (minus, centre, plus)]
    sums = (centre[0], centre[1], add(plus[0], minus[0]), add(plus[1], minus[1]))
    same, even, odd = [None] * 6, [None] * 6, [None] * 6
    for i in range(3):
        same[i] = add(*[mul(w, t) for w, t in zip(diag_weights(i, 0, 0) + diag_weights(i, 0, 1), sums)])
        even[i] = add(*[mul(w, t) for w, t in zip(diag_weights(i, 1, 0) + diag_weights(i, 1, 1), sums)])
    diff_d = sub(plus[2], minus[2])
    same[5] = mul(Q2, diff_d)
    even[5] = mul(Q3, diff_d)
    odd[3] = add(mul(Q2, sub(plus[0], minus[0])), mul(Q3, sub(plus[1], minus[1])))
    odd[4] = add(mul(Q2, centre[2]), mul(Q3, add(plus[2], minus[2])))
    return same, even, odd


def times_g(g, v):
    return (
        g[0] * v[0] + g[3] * v[1] + g[4] * v[2],
        g[3] * v[0] + g[1] * v[1] + g[5] * v[2],
        g[4] * v[0] + g[5] * v[1] + g[2] * v[2],
    )


def put_split(ref, row, slot, value):
    high = value.astype(jnp.bfloat16)
    low = (value - high.astype(jnp.float32)).astype(jnp.bfloat16)
    lanes = pl.ds(slot * NZ, NZ)
    ref[pl.ds(row, MODES), lanes] = high
    ref[pl.ds(row + MODES, MODES), lanes] = low


def contract(a, b):
    return lax.dot_general(a, b, (((1,), (1,)), ((), ())), preferred_element_type=jnp.float32)


def fold(raw):
    return raw[:MODES] + raw[MODES:]


def shifted_rows(plane):
    row = lax.broadcasted_iota(jnp.int32, plane.shape, 0)
    plus = jnp.where(row < CY - 1, pltpu.roll(plane, CY - 1, 0), 0.0)
    minus = jnp.where(row > 0, pltpu.roll(plane, 1, 0), 0.0)
    return minus, plus


def own_kernel(z_ref, e_ref, q_ref, ux_ref, vx_ref, uy_ref, vy_ref, s_ref, d_ref, same_ref, lower_ref, upper_ref, g_ref, lhs_ref, rhs_ref):
    lines = []
    for x in range(CX):
        plane = e_ref[x]
        minus, plus = shifted_rows(plane)
        lines.append(scalar_line(z_parts(minus), z_parts(plane), z_parts(plus)))
    for x in range(CX):
        for n in range(6):
            total = lines[x][0][n]
            if x + 1 < CX:
                total = add(total, lines[x + 1][1][n], lines[x + 1][2][n])
            if x > 0:
                total = sub(add(total, lines[x - 1][1][n]), lines[x - 1][2][n])
            g_ref[x, n] = 0.5 * total

    for i in range(3):
        for y in range(CY + 1):
            zero = jnp.zeros((MODES, NZ), jnp.float32)
            lower_ref[CX, i, y] = zero
            upper_ref[0, i, y] = zero

    def spread(x, carry):
        for y in range(CY):
            for i in range(3):
                _, s, d = z_parts(z_ref[i, x, y])
                s_ref[x, i, y] = s
                d_ref[x, i, y] = d
        for y in range(CY + 1):
            cells = [
                tuple((z_ref[i, x, t], s_ref[x, i, t], d_ref[x, i, t]) for i in range(3)) if 0 <= t < CY else None
                for t in (y - 1, y, y + 1)
            ]
            same, even, odd = line(*cells)
            for i in range(3):
                same_ref[x, i, y] = same[i]
                lower_ref[x, i, y] = add(even[i], odd[i])
                upper_ref[x + 1, i, y] = sub(even[i], odd[i])
        return carry

    lax.fori_loop(0, CX, spread, 0)

    def gather(x, total):
        for y in range(CY):
            e = e_ref[x, pl.ds(y, 1), :]
            v = [z_ref[i, x, y] for i in range(3)]
            g = [g_ref[x, n, pl.ds(y, 1), :] for n in range(6)]
            gv = times_g(g, v)
            for i in range(3):
                u = same_ref[x, i, y] + lower_ref[x + 1, i, y] + upper_ref[x, i, y]
                put_split(lhs_ref, 0, y * 3 + i, e * (HALF * v[i] - u) + gv[i])
                put_split(rhs_ref, 0, y * 3 + i, v[i])
        for i in range(3):
            uy_ref[i, x] = same_ref[x, i, CY] + lower_ref[x + 1, i, CY] + upper_ref[x, i, CY]
        return total + contract(lhs_ref[...], rhs_ref[...])

    raw = lax.fori_loop(0, CX, gather, jnp.zeros((2 * MODES, 2 * MODES), jnp.float32))
    q_ref[...] = raw
    for i in range(3):
        for y in range(CY):
            ux_ref[i, y] = upper_ref[CX, i, y]

    def weighted(x, y):
        e = e_ref[x, pl.ds(y, 1), :]
        return tuple(z_parts(e * z_ref[i, x, y]) for i in range(3))

    rim = [weighted(CX - 1, y) for y in range(CY)]
    for y in range(CY):
        _, even, odd = line(rim[y - 1] if y > 0 else None, rim[y], rim[y + 1] if y + 1 < CY else None, want0=False)
        for i in range(3):
            vx_ref[i, y] = sub(even[i], odd[i])
    edge = [line(weighted(x, CY - 1), None, None) for x in range(CX)]
    for x in range(CX):
        for i in range(3):
            total = edge[x][0][i]
            if x + 1 < CX:
                total = add(total, edge[x + 1][1][i], edge[x + 1][2][i])
            if x > 0:
                total = sub(add(total, edge[x - 1][1][i]), edge[x - 1][2][i])
            vy_ref[i, x] = total


def corner_parts(cell, e_here, e_there, sy):
    def stencil(v):
        parts = tuple(z_parts(t) for t in v)
        _, even, odd = line(None, None, parts) if sy > 0 else line(parts, None, None)
        return [sub(even[i], odd[i]) for i in range(3)]
    u = stencil(cell)
    w = stencil([e_here * t for t in cell])
    return [-(e_there * a + b) for a, b in zip(u, w)]


def halo_kernel(near_ref, z_ref, e_ref, q_ref, ux_ref, vx_ref, uy_ref, vy_ref, x_ref, yp_ref, ym_ref, own_ref, msg_ref,
                g_ref, lx_ref, rx_ref, ly_ref, ry_ref, lm_ref, lr_ref, rr_ref):
    ex, eyp, eym = 3 * CY * MODES, 3 * CX * MODES, 3 * MODES
    zx = lambda i, y: x_ref[pl.ds((i * CY + y) * MODES, MODES), :]
    zyp = lambda i, x: yp_ref[pl.ds((i * CX + x) * MODES, MODES), :]
    zym = lambda i: ym_ref[pl.ds(i * MODES, MODES), :]
    row = lax.broadcasted_iota(jnp.int32, (CY, NZ), 0)

    lines = []
    for x in range(CX):
        plus = jnp.where(row == CY - 1, yp_ref[pl.ds(eyp + x, 1), :], 0.0)
        minus = jnp.where(row == 0, ym_ref[pl.ds(eym + x, 1), :], 0.0)
        lines.append((minus, plus))
    side = x_ref[pl.ds(ex, CY), :]
    minus, plus = shifted_rows(side)
    far = scalar_line(z_parts(minus), z_parts(side), z_parts(plus))
    halo = [scalar_line(z_parts(m), None, z_parts(p)) for m, p in lines]
    minus, plus = shifted_rows(e_ref[CX - 1])
    back = scalar_line(z_parts(minus + lines[CX - 1][0]), z_parts(e_ref[CX - 1]), z_parts(plus + lines[CX - 1][1]))
    for x in range(CX):
        after = far if x + 1 == CX else halo[x + 1]
        for n in range(6):
            total = add(halo[x][0][n], after[1][n], after[2][n])
            if x > 0:
                total = sub(add(total, halo[x - 1][1][n]), halo[x - 1][2][n])
            g_ref[x, n] = 0.5 * total
    for n in range(6):
        g_ref[CX, n] = sub(back[1][n], back[2][n])

    def g_at(x, y):
        return [g_ref[x, n, pl.ds(y, 1), :] for n in range(6)]

    columns = [(CX - 1, y) for y in range(CY)] + [(x, y) for x in range(CX - 1) for y in (0, CY - 1)]
    for slot, (x, y) in enumerate(columns):
        v = [z_ref[i, x, y] for i in range(3)]
        gv = times_g(g_at(x, y), v)
        for i in range(3):
            put_split(lr_ref, 0, slot * 3 + i, gv[i])
            put_split(rr_ref, 0, slot * 3 + i, v[i])

    for y in range(CY):
        v = [zx(i, y) for i in range(3)]
        gv = times_g(g_at(CX, y), v)
        e = x_ref[pl.ds(ex + y, 1), :]
        for i in range(3):
            put_split(lx_ref, 0, y * 3 + i, -(e * ux_ref[i, y] + vx_ref[i, y]))
            put_split(lx_ref, 2 * MODES, y * 3 + i, gv[i])
            put_split(rx_ref, 0, y * 3 + i, v[i])
    for x in range(CX):
        e = yp_ref[pl.ds(eyp + x, 1), :]
        for i in range(3):
            put_split(ly_ref, 0, x * 3 + i, -(e * uy_ref[i, x] + vy_ref[i, x]))
            put_split(ry_ref, 0, x * 3 + i, zyp(i, x))

    last = CX - 1
    up = [zyp(i, last) for i in range(3)]
    down = [zym(i) for i in range(3)]
    e_up, e_down = yp_ref[pl.ds(eyp + last, 1), :], ym_ref[pl.ds(eym + last, 1), :]
    e_top, e_low = x_ref[pl.ds(ex + CY - 1, 1), :], x_ref[pl.ds(ex, 1), :]
    d_up = corner_parts(up, e_up, e_top, 1)
    d_down = corner_parts(down, e_down, e_low, -1)

    def corner_g(e, sy):
        _, even, odd = scalar_line(*((z_parts(e), None, None) if sy > 0 else (None, None, z_parts(e))))
        return [0.5 * add(even[n], odd[n]) for n in range(6)]

    g_up = times_g(corner_g(e_top, 1), up)
    g_down = times_g(corner_g(e_low, -1), down)
    for i in range(3):
        put_split(lm_ref, 0, i, d_up[i])
        put_split(lm_ref, 2 * MODES, i, d_down[i])
        put_split(lm_ref, 4 * MODES, i, g_up[i])
        put_split(lm_ref, 6 * MODES, i, g_down[i])
        put_split(lm_ref, 8 * MODES, i, down[i])

    wide = 2 * MODES
    k3 = 3 * NZ
    low, top = slice(0, k3), slice((CY - 1) * k3, CY * k3)
    last_y = slice(last * k3, (last + 1) * k3)
    raw_self = q_ref[...] + contract(lr_ref[...], rr_ref[...])
    raw_x = contract(lx_ref[...], rx_ref[...])
    raw_y = contract(ly_ref[...], ry_ref[...])
    raw_up = contract(lm_ref[0:wide], rx_ref[:, top])
    raw_down = contract(lm_ref[wide:2 * wide], rx_ref[:, low])
    raw_gup = contract(lm_ref[2 * wide:3 * wide], ry_ref[:, last_y])
    raw_gdown = contract(lm_ref[3 * wide:4 * wide], lm_ref[4 * wide:5 * wide])
    blocks = [raw_self, raw_y, raw_gup, raw_gdown, raw_x[:wide], raw_up, raw_down, raw_x[wide:]]
    tall = jnp.concatenate([fold(t) for t in blocks], axis=0)
    rows = tall.shape[0]
    tall = jnp.concatenate([tall, jnp.zeros((rows, NZ - wide), jnp.float32)], axis=1)
    lane = lax.broadcasted_iota(jnp.int32, (rows, NZ), 1)
    tall = jnp.where(lane < MODES, tall + pltpu.roll(tall, NZ - MODES, 1), 0.0)
    for shift in (MODES, 2 * MODES, 4 * MODES):
        tall = tall + pltpu.roll(tall, shift, 1)
    here, above, below, ahead = near_ref[4], near_ref[5], near_ref[3], near_ref[7]
    group = lax.broadcasted_iota(jnp.int32, (MODES, NZ), 1) // MODES

    def placed(entries, g):
        total = jnp.zeros((MODES, NZ), jnp.float32)
        for n, r, c in entries:
            total = total + jnp.where(group == jnp.where(r == g, c, -1), tall[n * MODES:(n + 1) * MODES], 0.0)
        return total

    entries = [(0, here, here), (1, here, above), (2, above, above), (3, below, below)]
    entries += [(4, here, ahead + GROUPS), (5, above, ahead + GROUPS), (6, below, ahead + GROUPS)]
    wide_rows = jnp.concatenate([placed(entries, g) for g in range(GROUPS)], axis=0)
    side_rows = jnp.concatenate([placed([(7, ahead, ahead + GROUPS)], g) for g in range(GROUPS)], axis=0)
    half = GROUPS * MODES
    turned = jnp.concatenate([wide_rows, jnp.zeros_like(wide_rows)], axis=0).T
    lane = lax.broadcasted_iota(jnp.int32, (half, NZ), 1)
    both = pltpu.roll(wide_rows + turned[:half], half, 1)
    own_ref[:, 0:NZ] = jnp.where(lane >= half, both, 0.0)
    own_ref[:, NZ:NZ + half] = pltpu.roll(wide_rows, half, 1)[:, :half]
    msg_ref[...] = jnp.where(lane < half, turned[half:], side_rows)


def vmem(n):
    return [pl.BlockSpec(memory_space=pltpu.VMEM)] * n


def f32(*shape):
    return jax.ShapeDtypeStruct(shape, jnp.float32)


def shards(modes, region, stiffness, coarse_group):
    levels = jnp.arange(stiffness.shape[0], dtype=jnp.int32)
    e = jnp.sum(jnp.where(region[..., None] == levels, stiffness, 0.0), axis=-1)
    z = jnp.transpose(modes, (1, 2, 3, 0, 4))
    zeros = jnp.zeros((4, NZ), jnp.float32)
    pay_x = jnp.concatenate([z[:, 0].reshape(-1, NZ), e[0]], axis=0)
    pay_yp = jnp.concatenate([z[:, :, 0].reshape(-1, NZ), e[:, 0], zeros], axis=0)
    pay_ym = jnp.concatenate([z[:, CX - 1, CY - 1].reshape(-1, NZ), e[:, CY - 1], zeros], axis=0)
    n_gx, n_gy = lax.axis_size("gx"), lax.axis_size("gy")
    got_x = lax.ppermute(pay_x, "gx", [(i + 1, i) for i in range(n_gx - 1)])
    got_yp = lax.ppermute(pay_yp, "gy", [(i + 1, i) for i in range(n_gy - 1)])
    got_ym = lax.ppermute(pay_ym, "gy", [(i, i + 1) for i in range(n_gy - 1)])
    group_pad = jnp.pad(coarse_group, 1, constant_values=-1)
    near = lax.dynamic_slice(group_pad, (lax.axis_index("gx"), lax.axis_index("gy")), (3, 3)).reshape(9)

    col = (MODES, NZ)
    k_own, k_x, k_y, k_rim = 3 * CY * NZ, 3 * CY * NZ, 3 * CX * NZ, 42 * NZ
    wide = 2 * MODES
    bf16 = jnp.bfloat16
    q, ux, vx, uy, vy = pl.pallas_call(
        own_kernel,
        out_shape=[f32(wide, wide), f32(3, CY, *col), f32(3, CY, *col), f32(3, CX, *col), f32(3, CX, *col)],
        in_specs=vmem(2),
        out_specs=vmem(5),
        scratch_shapes=[
            pltpu.VMEM((CX, 3, CY, *col), jnp.float32),
            pltpu.VMEM((CX, 3, CY, *col), jnp.float32),
            pltpu.VMEM((CX, 3, CY + 1, *col), jnp.float32),
            pltpu.VMEM((CX + 1, 3, CY + 1, *col), jnp.float32),
            pltpu.VMEM((CX + 1, 3, CY + 1, *col), jnp.float32),
            pltpu.VMEM((CX, 6, CY, NZ), jnp.float32),
            pltpu.VMEM((wide, k_own), bf16),
            pltpu.VMEM((wide, k_own), bf16),
        ],
        cost_estimate=pl.CostEstimate(flops=4_000_000_000, bytes_accessed=1_000_000, transcendentals=0),
        name="own",
    )(z, e)
    own, msg = pl.pallas_call(
        halo_kernel,
        out_shape=[f32(GROUPS * MODES, 3 * GROUPS * MODES), f32(GROUPS * MODES, NZ)],
        in_specs=[pl.BlockSpec(memory_space=pltpu.SMEM)] + vmem(10),
        out_specs=vmem(2),
        scratch_shapes=[
            pltpu.VMEM((CX + 1, 6, CY, NZ), jnp.float32),
            pltpu.VMEM((2 * wide, k_x), bf16),
            pltpu.VMEM((wide, k_x), bf16),
            pltpu.VMEM((wide, k_y), bf16),
            pltpu.VMEM((wide, k_y), bf16),
            pltpu.VMEM((5 * wide, 3 * NZ), bf16),
            pltpu.VMEM((wide, k_rim), bf16),
            pltpu.VMEM((wide, k_rim), bf16),
        ],
        cost_estimate=pl.CostEstimate(flops=500_000_000, bytes_accessed=500_000, transcendentals=0),
        name="halo",
    )(near, z, e, q, ux, vx, uy, vy, got_x, got_yp, got_ym)
    got = lax.ppermute(msg, "gx", [(i, i + 1) for i in range(n_gx - 1)])
    rows = own + jnp.pad(got, ((0, 0), (0, own.shape[1] - NZ)))
    parts = lax.all_to_all(rows.reshape(n_gy, -1, own.shape[1]), "gy", 0, 0, tiled=True)
    return jnp.sum(parts, axis=0)[None]


def solution(mesh):
    in_specs = (P(None, None, "gx", "gy", None), P("gx", "gy", None), P(), P())
    out_specs = P("gx", "gy", None)
    return jax.shard_map(shards, mesh=mesh, in_specs=in_specs, out_specs=out_specs, check_vma=False)
```

```python
import jax
import jax.numpy as jnp
from jax import lax
from jax.experimental import pallas as pl
from jax.experimental.pallas import tpu as pltpu
from jax.sharding import PartitionSpec as P

GROUPS = 4
MODES = 16
CX = 4
CY = 8
NZ = 128

beta_shear = 0.5
mass_share = 0.1

Q1 = 0.5 * beta_shear
Q2 = 0.25 * beta_shear / 2
Q3 = 0.125 * beta_shear / 3
DIAG = 7.0 + 2 * Q1 + 8 * Q2 + 8 * Q3
HALF = 0.5 * (mass_share + DIAG)

KZ = {(0, 0): (0.0, 0.5), (0, 1): (0.5, 0.25), (1, 0): (0.5, 0.25), (1, 1): (0.25, 0.125)}


def diag_weights(comp, ax, ay):
    c, s = KZ[(ax, ay)]
    m = ax + ay
    if (comp == 0 and ax) or (comp == 1 and ay):
        c += (0.0, Q1, Q2)[m]
        s += (Q1, Q2, Q3)[m]
    if comp == 2:
        s += (Q1, Q2, Q3)[m]
    return c, s


def add(*terms):
    terms = [t for t in terms if t is not None]
    if not terms:
        return None
    total = terms[0]
    for t in terms[1:]:
        total = total + t
    return total


def sub(a, b):
    if b is None:
        return a
    if a is None:
        return -b
    return a - b


def mul(k, a):
    return None if a is None or k == 0.0 else k * a


def z_parts(v):
    lane = lax.broadcasted_iota(jnp.int32, v.shape, 1)
    up = jnp.where(lane < NZ - 1, pltpu.roll(v, NZ - 1, 1), 0.0)
    down = jnp.where(lane > 0, pltpu.roll(v, 1, 1), 0.0)
    return v, up + down, up - down


NONE3 = (None, None, None)


def line(minus, centre, plus, want0=True, want1=True):
    minus, centre, plus = [(NONE3,) * 3 if t is None else t for t in (minus, centre, plus)]
    sum_c = [add(plus[i][0], minus[i][0]) for i in range(3)]
    sum_s = [add(plus[i][1], minus[i][1]) for i in range(3)]
    diff_dz = sub(plus[2][2], minus[2][2])
    diff_dy = sub(plus[1][2], minus[1][2])
    same, even, odd = [None] * 3, [None] * 3, [None] * 3
    for i in range(3):
        parts = (centre[i][0], centre[i][1], sum_c[i], sum_s[i])
        if want0:
            k = diag_weights(i, 0, 0) + diag_weights(i, 0, 1)
            same[i] = add(*[mul(w, t) for w, t in zip(k, parts)])
        if want1:
            k = diag_weights(i, 1, 0) + diag_weights(i, 1, 1)
            even[i] = add(*[mul(w, t) for w, t in zip(k, parts)])
    if want0:
        same[1] = add(same[1], mul(Q2, diff_dz))
        same[2] = add(same[2], mul(Q2, diff_dy))
    if want1:
        even[1] = add(even[1], mul(Q3, diff_dz))
        even[2] = add(even[2], mul(Q3, diff_dy))
        diff = [add(mul(Q2, sub(plus[i][0], minus[i][0])), mul(Q3, sub(plus[i][1], minus[i][1]))) for i in (0, 1)]
        odd[1] = diff[0]
        odd[0] = add(diff[1], mul(Q2, centre[2][2]), mul(Q3, add(plus[2][2], minus[2][2])))
        odd[2] = add(mul(Q2, centre[0][2]), mul(Q3, add(plus[0][2], minus[0][2])))
    return same, even, odd


def scalar_line(minus, centre, plus):
    minus, centre, plus = [NONE3 if t is None else t for t in (minus, centre, plus)]
    sums = (centre[0], centre[1], add(plus[0], minus[0]), add(plus[1], minus[1]))
    same, even, odd = [None] * 6, [None] * 6, [None] * 6
    for i in range(3):
        same[i] = add(*[mul(w, t) for w, t in zip(diag_weights(i, 0, 0) + diag_weights(i, 0, 1), sums)])
        even[i] = add(*[mul(w, t) for w, t in zip(diag_weights(i, 1, 0) + diag_weights(i, 1, 1), sums)])
    diff_d = sub(plus[2], minus[2])
    same[5] = mul(Q2, diff_d)
    even[5] = mul(Q3, diff_d)
    odd[3] = add(mul(Q2, sub(plus[0], minus[0])), mul(Q3, sub(plus[1], minus[1])))
    odd[4] = add(mul(Q2, centre[2]), mul(Q3, add(plus[2], minus[2])))
    return same, even, odd


def times_g(g, v):
    return (
        g[0] * v[0] + g[3] * v[1] + g[4] * v[2],
        g[3] * v[0] + g[1] * v[1] + g[5] * v[2],
        g[4] * v[0] + g[5] * v[1] + g[2] * v[2],
    )


def put_split(ref, row, slot, value):
    high = value.astype(jnp.bfloat16)
    low = (value - high.astype(jnp.float32)).astype(jnp.bfloat16)
    lanes = pl.ds(slot * NZ, NZ)
    ref[pl.ds(row, MODES), lanes] = high
    ref[pl.ds(row + MODES, MODES), lanes] = low


def contract(a, b):
    return lax.dot_general(a, b, (((1,), (1,)), ((), ())), preferred_element_type=jnp.float32)


def fold(raw):
    return raw[:MODES] + raw[MODES:]


def shifted_rows(plane):
    row = lax.broadcasted_iota(jnp.int32, plane.shape, 0)
    plus = jnp.where(row < CY - 1, pltpu.roll(plane, CY - 1, 0), 0.0)
    minus = jnp.where(row > 0, pltpu.roll(plane, 1, 0), 0.0)
    return minus, plus


def own_kernel(z_ref, e_ref, q_ref, ux_ref, vx_ref, uy_ref, vy_ref, s_ref, d_ref, same_ref, lower_ref, upper_ref, g_ref, lhs_ref, rhs_ref):
    lines = []
    for x in range(CX):
        plane = e_ref[x]
        minus, plus = shifted_rows(plane)
        lines.append(scalar_line(z_parts(minus), z_parts(plane), z_parts(plus)))
    for x in range(CX):
        for n in range(6):
            total = lines[x][0][n]
            if x + 1 < CX:
                total = add(total, lines[x + 1][1][n], lines[x + 1][2][n])
            if x > 0:
                total = sub(add(total, lines[x - 1][1][n]), lines[x - 1][2][n])
            g_ref[x, n] = 0.5 * total

    for i in range(3):
        for y in range(CY + 1):
            zero = jnp.zeros((MODES, NZ), jnp.float32)
            lower_ref[CX, i, y] = zero
            upper_ref[0, i, y] = zero

    def spread(x, carry):
        for y in range(CY):
            for i in range(3):
                _, s, d = z_parts(z_ref[i, x, y])
                s_ref[x, i, y] = s
                d_ref[x, i, y] = d
        for y in range(CY + 1):
            cells = [
                tuple((z_ref[i, x, t], s_ref[x, i, t], d_ref[x, i, t]) for i in range(3)) if 0 <= t < CY else None
                for t in (y - 1, y, y + 1)
            ]
            same, even, odd = line(*cells)
            for i in range(3):
                same_ref[x, i, y] = same[i]
                lower_ref[x, i, y] = add(even[i], odd[i])
                upper_ref[x + 1, i, y] = sub(even[i], odd[i])
        return carry

    lax.fori_loop(0, CX, spread, 0)

    def gather(x, total):
        for y in range(CY):
            e = e_ref[x, pl.ds(y, 1), :]
            v = [z_ref[i, x, y] for i in range(3)]
            g = [g_ref[x, n, pl.ds(y, 1), :] for n in range(6)]
            gv = times_g(g, v)
            for i in range(3):
                u = same_ref[x, i, y] + lower_ref[x + 1, i, y] + upper_ref[x, i, y]
                put_split(lhs_ref, 0, y * 3 + i, e * (HALF * v[i] - u) + gv[i])
                put_split(rhs_ref, 0, y * 3 + i, v[i])
        for i in range(3):
            uy_ref[i, x] = same_ref[x, i, CY] + lower_ref[x + 1, i, CY] + upper_ref[x, i, CY]
        return total + contract(lhs_ref[...], rhs_ref[...])

    raw = lax.fori_loop(0, CX, gather, jnp.zeros((2 * MODES, 2 * MODES), jnp.float32))
    q_ref[...] = raw
    for i in range(3):
        for y in range(CY):
            ux_ref[0, i, y] = upper_ref[CX, i, y]
            ux_ref[1, i, y] = lower_ref[0, i, y]

    def weighted(x, y):
        e = e_ref[x, pl.ds(y, 1), :]
        return tuple(z_parts(e * z_ref[i, x, y]) for i in range(3))

    for side, x in enumerate((CX - 1, 0)):
        rim = [weighted(x, y) for y in range(CY)]
        for y in range(CY):
            _, even, odd = line(rim[y - 1] if y > 0 else None, rim[y], rim[y + 1] if y + 1 < CY else None, want0=False)
            for i in range(3):
                vx_ref[side, i, y] = (add, sub)[side == 0](even[i], odd[i])
    edge = [line(weighted(x, CY - 1), None, None) for x in range(CX)]
    for x in range(CX):
        for i in range(3):
            total = edge[x][0][i]
            if x + 1 < CX:
                total = add(total, edge[x + 1][1][i], edge[x + 1][2][i])
            if x > 0:
                total = sub(add(total, edge[x - 1][1][i]), edge[x - 1][2][i])
            vy_ref[i, x] = total


SIDES = (0, 1)
EDGE = (CX - 1, 0)


def y_kernel(z_ref, e_ref, q_ref, uy_ref, vy_ref, yp_ref, ym_ref, raw_ref, cu_ref, cv_ref, cz_ref,
             g_ref, ly_ref, ry_ref, lr_ref, rr_ref):
    eyp, eym = 3 * CX * MODES, 6 * MODES
    row = lax.broadcasted_iota(jnp.int32, (CY, NZ), 0)
    halo = []
    for x in range(CX):
        plus = jnp.where(row == CY - 1, yp_ref[pl.ds(eyp + x, 1), :], 0.0)
        minus = jnp.where(row == 0, ym_ref[pl.ds(eym + x, 1), :], 0.0)
        halo.append(scalar_line(z_parts(minus), None, z_parts(plus)))
    for x in range(CX):
        for n in range(6):
            total = halo[x][0][n]
            if x + 1 < CX:
                total = add(total, halo[x + 1][1][n], halo[x + 1][2][n])
            if x > 0:
                total = sub(add(total, halo[x - 1][1][n]), halo[x - 1][2][n])
            g_ref[x, n] = 0.5 * total
    for slot, (x, y) in enumerate([(x, y) for x in range(CX) for y in (0, CY - 1)]):
        v = [z_ref[i, x, y] for i in range(3)]
        gv = times_g([g_ref[x, n, pl.ds(y, 1), :] for n in range(6)], v)
        for i in range(3):
            put_split(lr_ref, 0, slot * 3 + i, gv[i])
            put_split(rr_ref, 0, slot * 3 + i, v[i])
    for x in range(CX):
        e = yp_ref[pl.ds(eyp + x, 1), :]
        for i in range(3):
            put_split(ly_ref, 0, x * 3 + i, -(e * uy_ref[i, x] + vy_ref[i, x]))
            put_split(ry_ref, 0, x * 3 + i, yp_ref[pl.ds((i * CX + x) * MODES, MODES), :])
    raw_ref[0] = q_ref[...] + contract(lr_ref[...], rr_ref[...])
    raw_ref[1] = contract(ly_ref[...], ry_ref[...])
    for side in SIDES:
        x = EDGE[side]
        for n, sy in enumerate((1, -1)):
            if sy > 0:
                v = [yp_ref[pl.ds((i * CX + x) * MODES, MODES), :] for i in range(3)]
                e = yp_ref[pl.ds(eyp + x, 1), :]
            else:
                v = [ym_ref[pl.ds((side * 3 + i) * MODES, MODES), :] for i in range(3)]
                e = ym_ref[pl.ds(eym + x, 1), :]
            for out_ref, field in ((cu_ref, v), (cv_ref, [e * t for t in v])):
                parts = tuple(z_parts(t) for t in field)
                _, even, odd = line(None, None, parts, want0=False) if sy > 0 else line(parts, None, None, want0=False)
                for i in range(3):
                    out_ref[side, n, i] = (add, sub)[side == 0](even[i], odd[i])
            for i in range(3):
                put_split(cz_ref, (n * 2) * MODES, side * 3 + i, v[i])


def x_kernel(cg_ref, z_ref, raw_ref, ux_ref, vx_ref, cu_ref, cv_ref, cz_ref, first_ref, second_ref, out_ref,
             g_ref, lx_ref, rx_ref, lc_ref, lg_ref, lr_ref, rr_ref):
    a, b = lax.axis_index("gx"), lax.axis_index("gy")
    even_strip = a % 2 == 0
    wide = 2 * MODES

    def face(side, at):
        here, there = (first_ref[at, :], second_ref[at, :]) if side == 0 else (second_ref[at, :], first_ref[at, :])
        return jnp.where(even_strip, here, there)

    for slot, (side, y) in enumerate([(side, y) for side in SIDES for y in range(CY)]):
        for i in range(3):
            put_split(rr_ref, 0, slot * 3 + i, z_ref[i, EDGE[side], y])
    ex = 3 * CY * MODES
    for side in SIDES:
        plane = face(side, pl.ds(ex, CY))
        minus, plus = shifted_rows(plane)
        _, even, odd = scalar_line(z_parts(minus), z_parts(plane), z_parts(plus))
        beside = [0.5 * (add, sub)[side](even[n], odd[n]) for n in range(6)]
        row = lax.broadcasted_iota(jnp.int32, (CY, NZ), 0)
        ends = scalar_line(z_parts(jnp.where(row == 0, plane[CY - 1:], 0.0)), None, z_parts(jnp.where(row == 1, plane[:1], 0.0)))
        corner = [0.5 * (add, sub)[side](ends[1][n], ends[2][n]) for n in range(6)]
        for n in range(6):
            g_ref[side, n] = beside[n]
            g_ref[2 + side, n] = corner[n]
        for y in range(CY):
            v = [z_ref[i, EDGE[side], y] for i in range(3)]
            gv = times_g([g_ref[side, n, pl.ds(y, 1), :] for n in range(6)], v)
            e = face(side, pl.ds(ex + y, 1))
            for i in range(3):
                put_split(lr_ref, 0, (side * CY + y) * 3 + i, gv[i])
                put_split(lx_ref, side * wide, y * 3 + i, -(e * ux_ref[side, i, y] + vx_ref[side, i, y]))
                put_split(rx_ref, side * wide, y * 3 + i, face(side, pl.ds((i * CY + y) * MODES, MODES)))
        for n, y in enumerate((CY - 1, 0)):
            e = face(side, pl.ds(ex + y, 1))
            for i in range(3):
                put_split(lc_ref, (side * 2 + n) * wide, i, -(e * cu_ref[side, n, i] + cv_ref[side, n, i]))

    k3 = 3 * NZ
    blocks = [raw_ref[0] + contract(lr_ref[...], rr_ref[...]), raw_ref[1]]
    for n in range(2):
        for side in SIDES:
            v = [(cz_ref[pl.ds(n * wide, MODES), pl.ds((side * 3 + i) * NZ, NZ)].astype(jnp.float32)
                  + cz_ref[pl.ds(n * wide + MODES, MODES), pl.ds((side * 3 + i) * NZ, NZ)].astype(jnp.float32)) for i in range(3)]
            gv = times_g([g_ref[2 + side, m, pl.ds(n, 1), :] for m in range(6)], v)
            for i in range(3):
                put_split(lg_ref, n * wide, side * 3 + i, gv[i])
        blocks.append(contract(lg_ref[pl.ds(n * wide, wide), :], cz_ref[pl.ds(n * wide, wide), :]))
    for side in SIDES:
        rows = slice(side * wide, (side + 1) * wide)
        blocks.append(contract(lx_ref[rows], rx_ref[rows]))
        for n, y in enumerate((CY - 1, 0)):
            blocks.append(contract(lc_ref[pl.ds((side * 2 + n) * wide, wide), :], rx_ref[rows, y * k3:(y + 1) * k3]))
    tall = jnp.concatenate([fold(t) for t in blocks], axis=0)
    rows = tall.shape[0]
    tall = jnp.concatenate([tall, jnp.zeros((rows, NZ - wide), jnp.float32)], axis=1)
    lane = lax.broadcasted_iota(jnp.int32, (rows, NZ), 1)
    tall = jnp.where(lane < MODES, tall + pltpu.roll(tall, NZ - MODES, 1), 0.0)
    for shift in (MODES, 2 * MODES, 4 * MODES):
        tall = tall + pltpu.roll(tall, shift, 1)

    groups = cg_ref[...].astype(jnp.float32)
    at_y, at_x = [lax.broadcasted_iota(jnp.int32, groups.shape, axis) for axis in (0, 1)]

    def group_of(step_x, step_y):
        found = jnp.where((at_x == a + step_x) & (at_y == b + step_y), groups, 0.0)
        return jnp.sum(jnp.sum(found, axis=0, keepdims=True), axis=1, keepdims=True)

    here, ahead, behind, above, below = [group_of(*step) for step in ((0, 0), (1, 0), (-1, 0), (0, 1), (0, -1))]
    group = (lax.broadcasted_iota(jnp.int32, (MODES, NZ), 1) // MODES).astype(jnp.float32)

    def placed(entries):
        rows = []
        for g in range(GROUPS):
            total = jnp.zeros((MODES, NZ), jnp.float32)
            for n, r, c in entries:
                total = total + jnp.where(group == jnp.where(r == g, c, -1.0), tall[n * MODES:(n + 1) * MODES], 0.0)
            rows.append(total)
        return jnp.concatenate(rows, axis=0)

    mid = here + GROUPS
    own = placed([(0, here, mid), (1, here, above + GROUPS), (2, above, above + GROUPS), (3, below, below + GROUPS)])
    left = placed([(7, here, behind), (8, above, behind), (9, below, behind)])
    right = placed([(4, here, ahead), (5, above, ahead), (6, below, ahead)])
    half = GROUPS * MODES
    turned = jnp.concatenate([jnp.zeros_like(own), own], axis=0).T
    middle = left + own + turned[half:]
    n_owners, part = out_ref.shape[:2]
    for d in range(n_owners):
        out_ref[d, :, 0:NZ] = middle[d * part:(d + 1) * part]
        out_ref[d, :, NZ:NZ + half] = right[d * part:(d + 1) * part, :half]


def vmem(n):
    return [pl.BlockSpec(memory_space=pltpu.VMEM)] * n


def f32(*shape):
    return jax.ShapeDtypeStruct(shape, jnp.float32)


def shards(modes, region, stiffness, coarse_group):
    levels = jnp.arange(stiffness.shape[0], dtype=jnp.int32)
    e = jnp.sum(jnp.where(region[..., None] == levels, stiffness, 0.0), axis=-1)
    z = jnp.transpose(modes, (1, 2, 3, 0, 4))
    zeros = jnp.zeros((4, NZ), jnp.float32)
    n_gx, n_gy = lax.axis_size("gx"), lax.axis_size("gy")
    upper = jnp.concatenate([z[:, CX - 1].reshape(-1, NZ), e[CX - 1]], axis=0)
    lower = jnp.concatenate([z[:, 0].reshape(-1, NZ), e[0]], axis=0)
    even_strip = lax.axis_index("gx") % 2 == 0
    pay_yp = jnp.concatenate([z[:, :, 0].reshape(-1, NZ), e[:, 0], zeros], axis=0)
    pay_ym = jnp.concatenate([z[:, x, CY - 1].reshape(-1, NZ) for x in EDGE] + [e[:, CY - 1], zeros], axis=0)
    pairs = [[(i, i + 1) for i in range(start, n_gx - 1, 2)] for start in (0, 1)]
    swaps = [p + [(j, i) for i, j in p] for p in pairs]
    first = lax.ppermute(jnp.where(even_strip, upper, lower), "gx", swaps[0])
    second = lax.ppermute(jnp.where(even_strip, lower, upper), "gx", swaps[1])
    got_yp = lax.ppermute(pay_yp, "gy", [(i + 1, i) for i in range(n_gy - 1)])
    got_ym = lax.ppermute(pay_ym, "gy", [(i, i + 1) for i in range(n_gy - 1)])

    col = (MODES, NZ)
    wide = 2 * MODES
    bf16 = jnp.bfloat16
    V = pltpu.VMEM
    q, ux, vx, uy, vy = pl.pallas_call(
        own_kernel,
        out_shape=[f32(wide, wide), f32(2, 3, CY, *col), f32(2, 3, CY, *col), f32(3, CX, *col), f32(3, CX, *col)],
        in_specs=vmem(2),
        out_specs=vmem(5),
        scratch_shapes=[
            V((CX, 3, CY, *col), jnp.float32),
            V((CX, 3, CY, *col), jnp.float32),
            V((CX, 3, CY + 1, *col), jnp.float32),
            V((CX + 1, 3, CY + 1, *col), jnp.float32),
            V((CX + 1, 3, CY + 1, *col), jnp.float32),
            V((CX, 6, CY, NZ), jnp.float32),
            V((wide, 3 * CY * NZ), bf16),
            V((wide, 3 * CY * NZ), bf16),
        ],
        cost_estimate=pl.CostEstimate(flops=4_000_000_000, bytes_accessed=1_000_000, transcendentals=0),
        compiler_params=pltpu.CompilerParams(vmem_limit_bytes=16 * 2**20),
        name="own",
    )(z, e)
    raw, cu, cv, cz = pl.pallas_call(
        y_kernel,
        out_shape=[f32(2, wide, wide), f32(2, 2, 3, *col), f32(2, 2, 3, *col), jax.ShapeDtypeStruct((2 * wide, 6 * NZ), bf16)],
        in_specs=vmem(7),
        out_specs=vmem(4),
        scratch_shapes=[
            V((CX, 6, CY, NZ), jnp.float32),
            V((wide, 3 * CX * NZ), bf16),
            V((wide, 3 * CX * NZ), bf16),
            V((wide, 6 * CX * NZ), bf16),
            V((wide, 6 * CX * NZ), bf16),
        ],
        cost_estimate=pl.CostEstimate(flops=1_000_000_000, bytes_accessed=500_000, transcendentals=0),
        compiler_params=pltpu.CompilerParams(vmem_limit_bytes=16 * 2**20),
        name="beside_y",
    )(z, e, q, uy, vy, got_yp, got_ym)
    parts = pl.pallas_call(
        x_kernel,
        out_shape=f32(n_gy, GROUPS * MODES // n_gy, 3 * GROUPS * MODES),
        in_specs=vmem(10),
        out_specs=pl.BlockSpec(memory_space=pltpu.VMEM),
        scratch_shapes=[
            V((4, 6, CY, NZ), jnp.float32),
            V((2 * wide, 3 * CY * NZ), bf16),
            V((2 * wide, 3 * CY * NZ), bf16),
            V((4 * wide, 3 * NZ), bf16),
            V((2 * wide, 6 * NZ), bf16),
            V((wide, 6 * CY * NZ), bf16),
            V((wide, 6 * CY * NZ), bf16),
        ],
        cost_estimate=pl.CostEstimate(flops=1_000_000_000, bytes_accessed=500_000, transcendentals=0),
        compiler_params=pltpu.CompilerParams(vmem_limit_bytes=16 * 2**20),
        name="beside_x",
    )(coarse_group.T, z, raw, ux, vx, cu, cv, cz, first, second)
    parts = lax.all_to_all(parts, "gy", 0, 0, tiled=True)
    return jnp.sum(parts, axis=0)[None]


def solution(mesh):
    in_specs = (P(None, None, "gx", "gy", None), P("gx", "gy", None), P(), P())
    out_specs = P("gx", "gy", None)
    return jax.shard_map(shards, mesh=mesh, in_specs=in_specs, out_specs=out_specs, check_vma=False)
```

```python
import jax
import jax.numpy as jnp
from jax import lax
from jax.experimental import pallas as pl
from jax.experimental.pallas import tpu as pltpu
from jax.sharding import PartitionSpec as P

GROUPS = 4
MODES = 16
CX = 4
CY = 8
NZ = 128

beta_shear = 0.5
mass_share = 0.1

Q1 = 0.5 * beta_shear
Q2 = 0.25 * beta_shear / 2
Q3 = 0.125 * beta_shear / 3
DIAG = 7.0 + 2 * Q1 + 8 * Q2 + 8 * Q3
HALF = 0.5 * (mass_share + DIAG)

KZ = {(0, 0): (0.0, 0.5), (0, 1): (0.5, 0.25), (1, 0): (0.5, 0.25), (1, 1): (0.25, 0.125)}


def diag_weights(comp, ax, ay):
    c, s = KZ[(ax, ay)]
    m = ax + ay
    if (comp == 0 and ax) or (comp == 1 and ay):
        c += (0.0, Q1, Q2)[m]
        s += (Q1, Q2, Q3)[m]
    if comp == 2:
        s += (Q1, Q2, Q3)[m]
    return c, s


def add(*terms):
    terms = [t for t in terms if t is not None]
    if not terms:
        return None
    total = terms[0]
    for t in terms[1:]:
        total = total + t
    return total


def sub(a, b):
    if b is None:
        return a
    if a is None:
        return -b
    return a - b


def mul(k, a):
    return None if a is None or k == 0.0 else k * a


def z_parts(v):
    lane = lax.broadcasted_iota(jnp.int32, v.shape, 1)
    up = jnp.where(lane < NZ - 1, pltpu.roll(v, NZ - 1, 1), 0.0)
    down = jnp.where(lane > 0, pltpu.roll(v, 1, 1), 0.0)
    return v, up + down, up - down


NONE3 = (None, None, None)


def line(minus, centre, plus, want0=True, want1=True):
    minus, centre, plus = [(NONE3,) * 3 if t is None else t for t in (minus, centre, plus)]
    sum_c = [add(plus[i][0], minus[i][0]) for i in range(3)]
    sum_s = [add(plus[i][1], minus[i][1]) for i in range(3)]
    diff_dz = sub(plus[2][2], minus[2][2])
    diff_dy = sub(plus[1][2], minus[1][2])
    same, even, odd = [None] * 3, [None] * 3, [None] * 3
    for i in range(3):
        parts = (centre[i][0], centre[i][1], sum_c[i], sum_s[i])
        if want0:
            k = diag_weights(i, 0, 0) + diag_weights(i, 0, 1)
            same[i] = add(*[mul(w, t) for w, t in zip(k, parts)])
        if want1:
            k = diag_weights(i, 1, 0) + diag_weights(i, 1, 1)
            even[i] = add(*[mul(w, t) for w, t in zip(k, parts)])
    if want0:
        same[1] = add(same[1], mul(Q2, diff_dz))
        same[2] = add(same[2], mul(Q2, diff_dy))
    if want1:
        even[1] = add(even[1], mul(Q3, diff_dz))
        even[2] = add(even[2], mul(Q3, diff_dy))
        diff = [add(mul(Q2, sub(plus[i][0], minus[i][0])), mul(Q3, sub(plus[i][1], minus[i][1]))) for i in (0, 1)]
        odd[1] = diff[0]
        odd[0] = add(diff[1], mul(Q2, centre[2][2]), mul(Q3, add(plus[2][2], minus[2][2])))
        odd[2] = add(mul(Q2, centre[0][2]), mul(Q3, add(plus[0][2], minus[0][2])))
    return same, even, odd


def scalar_line(minus, centre, plus):
    minus, centre, plus = [NONE3 if t is None else t for t in (minus, centre, plus)]
    sums = (centre[0], centre[1], add(plus[0], minus[0]), add(plus[1], minus[1]))
    same, even, odd = [None] * 6, [None] * 6, [None] * 6
    for i in range(3):
        same[i] = add(*[mul(w, t) for w, t in zip(diag_weights(i, 0, 0) + diag_weights(i, 0, 1), sums)])
        even[i] = add(*[mul(w, t) for w, t in zip(diag_weights(i, 1, 0) + diag_weights(i, 1, 1), sums)])
    diff_d = sub(plus[2], minus[2])
    same[5] = mul(Q2, diff_d)
    even[5] = mul(Q3, diff_d)
    odd[3] = add(mul(Q2, sub(plus[0], minus[0])), mul(Q3, sub(plus[1], minus[1])))
    odd[4] = add(mul(Q2, centre[2]), mul(Q3, add(plus[2], minus[2])))
    return same, even, odd


def times_g(g, v):
    return (
        g[0] * v[0] + g[3] * v[1] + g[4] * v[2],
        g[3] * v[0] + g[1] * v[1] + g[5] * v[2],
        g[4] * v[0] + g[5] * v[1] + g[2] * v[2],
    )


def put_split(ref, row, slot, value):
    high = value.astype(jnp.bfloat16)
    low = (value - high.astype(jnp.float32)).astype(jnp.bfloat16)
    lanes = pl.ds(slot * NZ, NZ)
    ref[pl.ds(row, MODES), lanes] = high
    ref[pl.ds(row + MODES, MODES), lanes] = low


def contract(a, b):
    return lax.dot_general(a, b, (((1,), (1,)), ((), ())), preferred_element_type=jnp.float32)


def fold(raw):
    return raw[:MODES] + raw[MODES:]


def shifted_rows(plane):
    row = lax.broadcasted_iota(jnp.int32, plane.shape, 0)
    plus = jnp.where(row < CY - 1, pltpu.roll(plane, CY - 1, 0), 0.0)
    minus = jnp.where(row > 0, pltpu.roll(plane, 1, 0), 0.0)
    return minus, plus


def own_kernel(z_ref, e_ref, cg_in, q_ref, ux_ref, vx_ref, uy_ref, vy_ref, group_ref,
               s_ref, d_ref, same_ref, lower_ref, upper_ref, g_ref, lhs_ref, rhs_ref, cg_ref, sem):
    copy = pltpu.make_async_copy(cg_in, cg_ref, sem)
    copy.start()
    lines = []
    for x in range(CX):
        plane = e_ref[x]
        minus, plus = shifted_rows(plane)
        lines.append(scalar_line(z_parts(minus), z_parts(plane), z_parts(plus)))
    for x in range(CX):
        for n in range(6):
            total = lines[x][0][n]
            if x + 1 < CX:
                total = add(total, lines[x + 1][1][n], lines[x + 1][2][n])
            if x > 0:
                total = sub(add(total, lines[x - 1][1][n]), lines[x - 1][2][n])
            g_ref[x, n] = 0.5 * total

    for i in range(3):
        for y in range(CY + 1):
            zero = jnp.zeros((MODES, NZ), jnp.float32)
            lower_ref[CX, i, y] = zero
            upper_ref[0, i, y] = zero

    def spread(x, carry):
        for y in range(CY):
            for i in range(3):
                _, s, d = z_parts(z_ref[i, x, y])
                s_ref[x, i, y] = s
                d_ref[x, i, y] = d
        for y in range(CY + 1):
            cells = [
                tuple((z_ref[i, x, t], s_ref[x, i, t], d_ref[x, i, t]) for i in range(3)) if 0 <= t < CY else None
                for t in (y - 1, y, y + 1)
            ]
            same, even, odd = line(*cells)
            for i in range(3):
                same_ref[x, i, y] = same[i]
                lower_ref[x, i, y] = add(even[i], odd[i])
                upper_ref[x + 1, i, y] = sub(even[i], odd[i])
        return carry

    lax.fori_loop(0, CX, spread, 0)

    def gather(x, total):
        for y in range(CY):
            e = e_ref[x, pl.ds(y, 1), :]
            v = [z_ref[i, x, y] for i in range(3)]
            g = [g_ref[x, n, pl.ds(y, 1), :] for n in range(6)]
            gv = times_g(g, v)
            for i in range(3):
                u = same_ref[x, i, y] + lower_ref[x + 1, i, y] + upper_ref[x, i, y]
                put_split(lhs_ref, 0, y * 3 + i, e * (HALF * v[i] - u) + gv[i])
                put_split(rhs_ref, 0, y * 3 + i, v[i])
        for i in range(3):
            uy_ref[i, x] = same_ref[x, i, CY] + lower_ref[x + 1, i, CY] + upper_ref[x, i, CY]
        return total + contract(lhs_ref[...], rhs_ref[...])

    raw = lax.fori_loop(0, CX, gather, jnp.zeros((2 * MODES, 2 * MODES), jnp.float32))
    q_ref[...] = raw
    for i in range(3):
        for y in range(CY):
            ux_ref[0, i, y] = upper_ref[CX, i, y]
            ux_ref[1, i, y] = lower_ref[0, i, y]

    def weighted(x, y):
        e = e_ref[x, pl.ds(y, 1), :]
        return tuple(z_parts(e * z_ref[i, x, y]) for i in range(3))

    for side, x in enumerate((CX - 1, 0)):
        rim = [weighted(x, y) for y in range(CY)]
        for y in range(CY):
            _, even, odd = line(rim[y - 1] if y > 0 else None, rim[y], rim[y + 1] if y + 1 < CY else None, want0=False)
            for i in range(3):
                vx_ref[side, i, y] = (add, sub)[side == 0](even[i], odd[i])
    edge = [line(weighted(x, CY - 1), None, None) for x in range(CX)]
    for x in range(CX):
        for i in range(3):
            total = edge[x][0][i]
            if x + 1 < CX:
                total = add(total, edge[x + 1][1][i], edge[x + 1][2][i])
            if x > 0:
                total = sub(add(total, edge[x - 1][1][i]), edge[x - 1][2][i])
            vy_ref[i, x] = total

    copy.wait()
    groups = cg_ref[...].astype(jnp.float32)
    at_y, at_x = [lax.broadcasted_iota(jnp.int32, groups.shape, axis) for axis in (0, 1)]
    a, b = lax.axis_index("gx"), lax.axis_index("gy")
    for n, (step_x, step_y) in enumerate(((0, 0), (1, 0), (-1, 0), (0, 1), (0, -1))):
        found = jnp.where((at_x == a + step_x) & (at_y == b + step_y), groups, 0.0)
        one = jnp.sum(jnp.sum(found, axis=0, keepdims=True), axis=1, keepdims=True)
        group_ref[pl.ds(n, 1), :] = jnp.broadcast_to(one, (1, NZ))


SIDES = (0, 1)
EDGE = (CX - 1, 0)


def y_kernel(z_ref, q_ref, uy_ref, vy_ref, chip_ref, cross_ref, raw_ref, cu_ref, cv_ref, cz_ref,
             g_ref, ly_ref, ry_ref, lr_ref, rr_ref):
    even_column = lax.axis_index("gy") % 2 == 0
    ends = 3 * CX * MODES

    def face(upper, at):
        here, there = (chip_ref[at, :], cross_ref[at, :]) if upper else (cross_ref[at, :], chip_ref[at, :])
        return jnp.where(even_column, here, there)

    def column(upper, x):
        return [face(upper, pl.ds((i * CX + x) * MODES, MODES)) for i in range(3)], face(upper, pl.ds(ends + x, 1))

    row = lax.broadcasted_iota(jnp.int32, (CY, NZ), 0)
    halo = []
    for x in range(CX):
        plus = jnp.where(row == CY - 1, face(True, pl.ds(ends + x, 1)), 0.0)
        minus = jnp.where(row == 0, face(False, pl.ds(ends + x, 1)), 0.0)
        halo.append(scalar_line(z_parts(minus), None, z_parts(plus)))
    for x in range(CX):
        for n in range(6):
            total = halo[x][0][n]
            if x + 1 < CX:
                total = add(total, halo[x + 1][1][n], halo[x + 1][2][n])
            if x > 0:
                total = sub(add(total, halo[x - 1][1][n]), halo[x - 1][2][n])
            g_ref[x, n] = 0.5 * total
    for slot, (x, y) in enumerate([(x, y) for x in range(CX) for y in (0, CY - 1)]):
        v = [z_ref[i, x, y] for i in range(3)]
        gv = times_g([g_ref[x, n, pl.ds(y, 1), :] for n in range(6)], v)
        for i in range(3):
            put_split(lr_ref, 0, slot * 3 + i, gv[i])
            put_split(rr_ref, 0, slot * 3 + i, v[i])
    for x in range(CX):
        v, e = column(True, x)
        for i in range(3):
            put_split(ly_ref, 0, x * 3 + i, -(e * uy_ref[i, x] + vy_ref[i, x]))
            put_split(ry_ref, 0, x * 3 + i, v[i])
    raw_ref[0] = q_ref[...] + contract(lr_ref[...], rr_ref[...])
    raw_ref[1] = contract(ly_ref[...], ry_ref[...])
    for side in SIDES:
        x = EDGE[side]
        for n, sy in enumerate((1, -1)):
            v, e = column(sy > 0, x)
            for out_ref, field in ((cu_ref, v), (cv_ref, [e * t for t in v])):
                parts = tuple(z_parts(t) for t in field)
                _, even, odd = line(None, None, parts, want0=False) if sy > 0 else line(parts, None, None, want0=False)
                for i in range(3):
                    out_ref[side, n, i] = (add, sub)[side == 0](even[i], odd[i])
            for i in range(3):
                put_split(cz_ref, (n * 2) * MODES, side * 3 + i, v[i])


def x_kernel(group_ref, z_ref, raw_ref, ux_ref, vx_ref, cu_ref, cv_ref, cz_ref, first_ref, second_ref, out_ref,
             g_ref, lx_ref, rx_ref, lc_ref, lg_ref, lr_ref, rr_ref):
    even_strip = lax.axis_index("gx") % 2 == 0
    wide = 2 * MODES

    def face(side, at):
        here, there = (first_ref[at, :], second_ref[at, :]) if side == 0 else (second_ref[at, :], first_ref[at, :])
        return jnp.where(even_strip, here, there)

    for slot, (side, y) in enumerate([(side, y) for side in SIDES for y in range(CY)]):
        for i in range(3):
            put_split(rr_ref, 0, slot * 3 + i, z_ref[i, EDGE[side], y])
    ex = 3 * CY * MODES
    for side in SIDES:
        plane = face(side, pl.ds(ex, CY))
        minus, plus = shifted_rows(plane)
        _, even, odd = scalar_line(z_parts(minus), z_parts(plane), z_parts(plus))
        beside = [0.5 * (add, sub)[side](even[n], odd[n]) for n in range(6)]
        row = lax.broadcasted_iota(jnp.int32, (CY, NZ), 0)
        ends = scalar_line(z_parts(jnp.where(row == 0, plane[CY - 1:], 0.0)), None, z_parts(jnp.where(row == 1, plane[:1], 0.0)))
        corner = [0.5 * (add, sub)[side](ends[1][n], ends[2][n]) for n in range(6)]
        for n in range(6):
            g_ref[side, n] = beside[n]
            g_ref[2 + side, n] = corner[n]
        for y in range(CY):
            v = [z_ref[i, EDGE[side], y] for i in range(3)]
            gv = times_g([g_ref[side, n, pl.ds(y, 1), :] for n in range(6)], v)
            e = face(side, pl.ds(ex + y, 1))
            for i in range(3):
                put_split(lr_ref, 0, (side * CY + y) * 3 + i, gv[i])
                put_split(lx_ref, side * wide, y * 3 + i, -(e * ux_ref[side, i, y] + vx_ref[side, i, y]))
                put_split(rx_ref, side * wide, y * 3 + i, face(side, pl.ds((i * CY + y) * MODES, MODES)))
        for n, y in enumerate((CY - 1, 0)):
            e = face(side, pl.ds(ex + y, 1))
            for i in range(3):
                put_split(lc_ref, (side * 2 + n) * wide, i, -(e * cu_ref[side, n, i] + cv_ref[side, n, i]))

    k3 = 3 * NZ
    blocks = [raw_ref[0] + contract(lr_ref[...], rr_ref[...]), raw_ref[1]]
    for n in range(2):
        for side in SIDES:
            v = [(cz_ref[pl.ds(n * wide, MODES), pl.ds((side * 3 + i) * NZ, NZ)].astype(jnp.float32)
                  + cz_ref[pl.ds(n * wide + MODES, MODES), pl.ds((side * 3 + i) * NZ, NZ)].astype(jnp.float32)) for i in range(3)]
            gv = times_g([g_ref[2 + side, m, pl.ds(n, 1), :] for m in range(6)], v)
            for i in range(3):
                put_split(lg_ref, n * wide, side * 3 + i, gv[i])
        blocks.append(contract(lg_ref[pl.ds(n * wide, wide), :], cz_ref[pl.ds(n * wide, wide), :]))
    for side in SIDES:
        rows = slice(side * wide, (side + 1) * wide)
        blocks.append(contract(lx_ref[rows], rx_ref[rows]))
        for n, y in enumerate((CY - 1, 0)):
            blocks.append(contract(lc_ref[pl.ds((side * 2 + n) * wide, wide), :], rx_ref[rows, y * k3:(y + 1) * k3]))
    tall = jnp.concatenate([fold(t) for t in blocks], axis=0)
    rows = tall.shape[0]
    tall = jnp.concatenate([tall, jnp.zeros((rows, NZ - wide), jnp.float32)], axis=1)
    lane = lax.broadcasted_iota(jnp.int32, (rows, NZ), 1)
    tall = jnp.where(lane < MODES, tall + pltpu.roll(tall, NZ - MODES, 1), 0.0)
    for shift in (MODES, 2 * MODES, 4 * MODES):
        tall = tall + pltpu.roll(tall, shift, 1)

    here, ahead, behind, above, below = [group_ref[pl.ds(n, 1), :] for n in range(5)]
    group = (lax.broadcasted_iota(jnp.int32, (MODES, NZ), 1) // MODES).astype(jnp.float32)

    def placed(entries):
        rows = []
        for g in range(GROUPS):
            total = jnp.zeros((MODES, NZ), jnp.float32)
            for n, r, c in entries:
                total = total + jnp.where(group == jnp.where(r == g, c, -1.0), tall[n * MODES:(n + 1) * MODES], 0.0)
            rows.append(total)
        return jnp.concatenate(rows, axis=0)

    mid = here + GROUPS
    own = placed([(0, here, mid), (1, here, above + GROUPS), (2, above, above + GROUPS), (3, below, below + GROUPS)])
    left = placed([(7, here, behind), (8, above, behind), (9, below, behind)])
    right = placed([(4, here, ahead), (5, above, ahead), (6, below, ahead)])
    half = GROUPS * MODES
    turned = jnp.concatenate([jnp.zeros_like(own), own], axis=0).T
    middle = left + own + turned[half:]
    n_owners, part = out_ref.shape[:2]
    for d in range(n_owners):
        out_ref[d, :, 0:NZ] = middle[d * part:(d + 1) * part]
        out_ref[d, :, NZ:NZ + half] = right[d * part:(d + 1) * part, :half]


def vmem(n):
    return [pl.BlockSpec(memory_space=pltpu.VMEM)] * n


def f32(*shape):
    return jax.ShapeDtypeStruct(shape, jnp.float32)


def shards(modes, region, stiffness, coarse_group):
    levels = jnp.arange(stiffness.shape[0], dtype=jnp.int32)
    e = jnp.sum(jnp.where(region[..., None] == levels, stiffness, 0.0), axis=-1)
    z = jnp.transpose(modes, (1, 2, 3, 0, 4))
    zeros = jnp.zeros((4, NZ), jnp.float32)
    n_gx, n_gy = lax.axis_size("gx"), lax.axis_size("gy")
    upper = jnp.concatenate([z[:, CX - 1].reshape(-1, NZ), e[CX - 1]], axis=0)
    lower = jnp.concatenate([z[:, 0].reshape(-1, NZ), e[0]], axis=0)
    even_strip = lax.axis_index("gx") % 2 == 0
    even_column = lax.axis_index("gy") % 2 == 0
    above, below = [jnp.concatenate([z[:, :, y].reshape(-1, NZ), e[:, y], zeros], axis=0) for y in (CY - 1, 0)]

    def swaps(count, start):
        pairs = [(i, i + 1) for i in range(start, count - 1, 2)]
        return pairs + [(j, i) for i, j in pairs]

    chip = lax.ppermute(jnp.where(even_column, above, below), "gy", swaps(n_gy, 0))
    first = lax.ppermute(jnp.where(even_strip, upper, lower), "gx", swaps(n_gx, 0))
    second = lax.ppermute(jnp.where(even_strip, lower, upper), "gx", swaps(n_gx, 1))
    cross = lax.ppermute(jnp.where(even_column, below, above), "gy", swaps(n_gy, 1))

    col = (MODES, NZ)
    wide = 2 * MODES
    bf16 = jnp.bfloat16
    V = pltpu.VMEM
    q, ux, vx, uy, vy, group = pl.pallas_call(
        own_kernel,
        out_shape=[f32(wide, wide), f32(2, 3, CY, *col), f32(2, 3, CY, *col), f32(3, CX, *col), f32(3, CX, *col), f32(8, NZ)],
        in_specs=vmem(2) + [pl.BlockSpec(memory_space=pltpu.HBM)],
        out_specs=vmem(6),
        scratch_shapes=[
            V((CX, 3, CY, *col), jnp.float32),
            V((CX, 3, CY, *col), jnp.float32),
            V((CX, 3, CY + 1, *col), jnp.float32),
            V((CX + 1, 3, CY + 1, *col), jnp.float32),
            V((CX + 1, 3, CY + 1, *col), jnp.float32),
            V((CX, 6, CY, NZ), jnp.float32),
            V((wide, 3 * CY * NZ), bf16),
            V((wide, 3 * CY * NZ), bf16),
            V(coarse_group.T.shape, jnp.int32),
            pltpu.SemaphoreType.DMA,
        ],
        cost_estimate=pl.CostEstimate(flops=4_000_000_000, bytes_accessed=1_000_000, transcendentals=0),
        compiler_params=pltpu.CompilerParams(vmem_limit_bytes=16 * 2**20),
        name="own",
    )(z, e, coarse_group.T)
    raw, cu, cv, cz = pl.pallas_call(
        y_kernel,
        out_shape=[f32(2, wide, wide), f32(2, 2, 3, *col), f32(2, 2, 3, *col), jax.ShapeDtypeStruct((2 * wide, 6 * NZ), bf16)],
        in_specs=vmem(6),
        out_specs=vmem(4),
        scratch_shapes=[
            V((CX, 6, CY, NZ), jnp.float32),
            V((wide, 3 * CX * NZ), bf16),
            V((wide, 3 * CX * NZ), bf16),
            V((wide, 6 * CX * NZ), bf16),
            V((wide, 6 * CX * NZ), bf16),
        ],
        cost_estimate=pl.CostEstimate(flops=1_000_000_000, bytes_accessed=500_000, transcendentals=0),
        compiler_params=pltpu.CompilerParams(vmem_limit_bytes=16 * 2**20),
        name="beside_y",
    )(z, q, uy, vy, chip, cross)
    parts = pl.pallas_call(
        x_kernel,
        out_shape=f32(n_gy, GROUPS * MODES // n_gy, 3 * GROUPS * MODES),
        in_specs=vmem(10),
        out_specs=pl.BlockSpec(memory_space=pltpu.VMEM),
        scratch_shapes=[
            V((4, 6, CY, NZ), jnp.float32),
            V((2 * wide, 3 * CY * NZ), bf16),
            V((2 * wide, 3 * CY * NZ), bf16),
            V((4 * wide, 3 * NZ), bf16),
            V((2 * wide, 6 * NZ), bf16),
            V((wide, 6 * CY * NZ), bf16),
            V((wide, 6 * CY * NZ), bf16),
        ],
        cost_estimate=pl.CostEstimate(flops=1_000_000_000, bytes_accessed=500_000, transcendentals=0),
        compiler_params=pltpu.CompilerParams(vmem_limit_bytes=16 * 2**20),
        name="beside_x",
    )(group, z, raw, ux, vx, cu, cv, cz, first, second)
    parts = lax.all_to_all(parts, "gy", 0, 0, tiled=True)
    return jnp.sum(parts, axis=0)[None]


def solution(mesh):
    in_specs = (P(None, None, "gx", "gy", None), P("gx", "gy", None), P(), P())
    out_specs = P("gx", "gy", None)
    return jax.shard_map(shards, mesh=mesh, in_specs=in_specs, out_specs=out_specs, check_vma=False)
```
